32 devices in a mesh: ep: 4 (over y, x), grp: 8 (over z, core).
Axes of the slice: x: 2, y: 2, z: 4, core: 2. Of those that a mesh axis runs over, the one named last changes fastest.
Arguments:
- tokens: bfloat16 [4096, 4096], P(('ep', 'grp')), may hold values from -6 to 6
- expert_ids: int32 [4096, 8], P(('ep', 'grp')), may hold values from 0 to 127, all different within a row; in each aligned block of 128 rows (0 to 127, 128 to 255, ...) at most 16 rows name the same one
- combine: float32 [4096, 8], P(('ep', 'grp')), may hold values from 0.05 to 1
- w_gate: bfloat16 [4096, 1280], P(None, 'ep'), may hold values from -0.09375 to 0.09375
- w_up: bfloat16 [4096, 1280], P(None, 'ep'), may hold values from -0.09375 to 0.09375
- w_down: bfloat16 [1280, 4096], P('ep'), may hold values from -0.15625 to 0.15625
- bias: float32 [128], replicated, may hold values from -3 to 3
Outputs:
- mixed: bfloat16 [4096, 4096], P(('ep', 'grp'))
- new_bias: float32 [128], replicated
The draws below stay inside these ranges and needn't reach their ends.
Inputs may be any that keep to these rules, and one draw needn't show every extreme that they name: `expert_ids`: each row names 8 different experts. Among the rows of one device no expert is named more than 16 times, a bound that some block reaches.
All inputs are finite; a program needn't handle non-finite values.
Results may differ from the reference program's by a relative error of at most 0.0057.
Values may be sent and summed in bfloat16 or wider, within the bound.
A program may use at most 64 MiB of HBM per device.

```python
import math
import jax
import jax.numpy as jnp
import numpy as np
from jax import lax

D = 4096
NEXP = 128
TOPK = 8
FF_WIN = 1280
SPLIT = 4
TOK_DEV = 128
CAP = 16
FF_DEV = 320
E_WIN = 1
TOKENS = 4096


def block_scale(own_key, extent, split, low, high):
    factor_of, own = 1.0, jax.random.fold_in(own_key, 6)
    for axis_at, parts in split:
        heights = jnp.exp(jax.random.uniform(jax.random.fold_in(own, axis_at), (parts,), jnp.float32, low / len(split), high / len(split)))
        factor_of = factor_of * jnp.repeat(heights, extent[axis_at] // parts).reshape([-1 if axis == axis_at else 1 for axis in range(len(extent))])
    return factor_of


def routed_block(stream_key, own, number, rows, count, top, reach, skew):
    order = jax.random.permutation(stream_key, count)
    packed, ordinary = shares(count, rows * top, reach, skew, True), shares(count, rows * top, reach, skew, False)
    places = jnp.arange(count)

    def named(tallies, turn):
        used = int((tallies > 0).sum())
        fixed = max(1, used // 4)
        passed = fixed + (places - fixed + turn * (used - fixed)) % max(1, count - fixed)
        return jnp.zeros((count,), jnp.int32).at[order[jnp.where(places < fixed, places, passed)]].set(jnp.asarray(tallies, jnp.int32))

    tallies = jnp.where(number % 4 == 0, named(packed, number // 4), named(ordinary, number - number // 4 - 1))
    mixed = jax.random.permutation(jax.random.fold_in(own, 3), count)
    source_of, sink = mixed[0:count // 2 * 2:2], mixed[1:count // 2 * 2:2]
    slack = jnp.minimum(tallies[source_of] - 1, reach - tallies[sink]) // 2
    slack = jnp.where((source_of == order[0]) | (sink == order[0]) | (tallies[sink] == 0), 0, jnp.maximum(slack, 0))
    passed = jax.random.randint(jax.random.fold_in(own, 4), (count // 2,), 0, 1 << 20) % (slack + 1)
    tallies = tallies.at[source_of].add(-passed).at[sink].add(passed)
    members = jnp.searchsorted(jnp.cumsum(tallies), jnp.arange(rows * top), side="right").astype(jnp.int32)
    listing = members.reshape(top, rows).T
    listing = listing[jax.random.permutation(jax.random.fold_in(own, 1), rows)]
    turn = jax.random.randint(jax.random.fold_in(own, 2), (rows, 1), 0, top)
    return jnp.take_along_axis(listing, (jnp.arange(top)[None, :] + turn) % top, axis=1)


def shares(amount, total, reach, lean, full):
    weights = [(1 << 20) // math.isqrt(standing ** lean) + 1 for standing in range(1, amount + 1)]
    largest = reach if full else min(reach, max(-(-total // amount), total * weights[0] // sum(weights)))
    least = 1 if total - largest >= amount - 1 else 0
    counts, rest = [largest] + [least] * (amount - 1), total - largest - least * (amount - 1)
    while rest > 0:
        free = [i for i in range(1, amount) if counts[i] < largest] or [i for i in range(1, amount) if counts[i] < reach]
        pool, remaining = sum([weights[i] for i in free]), rest
        for i in free:
            addition = min(reach - counts[i], max(1, remaining * weights[i] // pool), rest)
            counts[i] = counts[i] + addition
            rest = rest - addition
    return np.array(counts)


def noise(own_key, dims, deviation, most, pieces=(), kind=jnp.bfloat16):
    gain = block_scale(own_key, dims, pieces, -0.22, 0.18) if pieces else 1.0
    entries = jax.random.normal(own_key, dims, jnp.float32) * deviation * gain
    return jnp.minimum(jnp.maximum(entries, -most), most).astype(kind)


def setup_inputs(seed: int = 0) -> dict:
    arg_keys = jax.random.split(jax.random.key(seed), 8)
    tokens = noise(arg_keys[0], (TOKENS, D), 1.0, 6.0, ((0, 32),))
    expert_ids_keys = jax.random.split(jax.random.fold_in(arg_keys[1], 1), TOKENS // TOK_DEV)
    expert_ids_turns = jax.random.permutation(jax.random.fold_in(arg_keys[1], 3), TOKENS // TOK_DEV)
    expert_ids = jax.vmap(lambda own, number: routed_block(jax.random.fold_in(arg_keys[1], 2), own, number, TOK_DEV, NEXP, TOPK, CAP, 2))(expert_ids_keys, expert_ids_turns).reshape((TOKENS, TOPK))
    combine = jnp.clip(jnp.exp(math.log(1.0) - 2.9957323 * jax.random.uniform(arg_keys[2], (TOKENS, TOPK), jnp.float32) ** block_scale(arg_keys[2], (TOKENS, TOPK), ((0, 32),), -0.2, 0.2)), 0.05, 1.0)
    w_gate = noise(arg_keys[3], (D, E_WIN * FF_WIN), D ** -0.5, 0.09375, ((1, 4),))
    w_up = noise(arg_keys[4], (D, E_WIN * FF_WIN), D ** -0.5, 0.09375, ((1, 4),))
    w_down = noise(arg_keys[5], (E_WIN * FF_WIN, D), FF_WIN ** -0.5, 0.15625, ((0, 4),))
    bias = noise(arg_keys[6], (NEXP,), 0.5, 3.0, (), jnp.float32)
    return {"tokens": tokens, "expert_ids": expert_ids, "combine": combine, "w_gate": w_gate, "w_up": w_up, "w_down": w_down, "bias": bias}


def reference(tokens, expert_ids, combine, w_gate, w_up, w_down, bias):
    blocks = tokens.shape[0] // TOK_DEV
    picks = expert_ids.reshape(blocks, TOK_DEV * TOPK)
    window = jnp.arange(E_WIN, dtype=jnp.int32)
    hit = (picks[:, :, None] == window[None, None, :]).astype(jnp.int32)
    ranks = jnp.cumsum(hit, axis=1) - 1
    slot = lax.optimization_barrier(jnp.sum(hit * ranks, axis=2))
    inside = lax.optimization_barrier(jnp.sum(hit, axis=2))
    block_idx = jnp.arange(blocks, dtype=jnp.int32)[:, None]
    total_slots = E_WIN * blocks * CAP
    dest = jnp.where(inside > 0, (picks * blocks + block_idx) * CAP + slot, total_slots).reshape(-1).astype(jnp.int32)
    token_of = (jnp.arange(blocks * TOK_DEV * TOPK, dtype=jnp.int32) // TOPK).astype(jnp.int32)
    source = jnp.full((total_slots + 1,), tokens.shape[0], jnp.int32).at[dest].set(token_of)[:total_slots]
    weight = jnp.zeros((total_slots + 1,), jnp.float32).at[dest].set(combine.reshape(-1).astype(jnp.float32))[:total_slots]
    padded = jnp.concatenate([tokens, jnp.zeros((1, tokens.shape[1]), tokens.dtype)], axis=0)
    rows_all = padded[source].reshape(E_WIN, blocks * CAP, tokens.shape[1])

    def expert(index):
        rows = rows_all[index]
        total = jnp.zeros((rows.shape[0], tokens.shape[1]), jnp.float32)
        for piece in range(SPLIT):
            start = index * FF_WIN + piece * FF_DEV
            g_cols = lax.dynamic_slice_in_dim(w_gate, start, FF_DEV, 1)
            u_cols = lax.dynamic_slice_in_dim(w_up, start, FF_DEV, 1)
            d_rows = lax.dynamic_slice_in_dim(w_down, start, FF_DEV, 0)
            gate = jnp.dot(rows, g_cols, preferred_element_type=jnp.float32)
            upval = jnp.dot(rows, u_cols, preferred_element_type=jnp.float32)
            hidden = (jax.nn.silu(gate) * upval).astype(jnp.bfloat16)
            part = jnp.dot(hidden, d_rows, preferred_element_type=jnp.float32).astype(jnp.bfloat16)
            total = total + part.astype(jnp.float32)
        return total
    outputs = lax.map(expert, jnp.arange(E_WIN, dtype=jnp.int32)).reshape(total_slots, tokens.shape[1])
    mixed = jnp.zeros((tokens.shape[0] + 1, tokens.shape[1]), jnp.float32).at[source].add(outputs * weight[:, None])
    mixed = mixed[:tokens.shape[0]].astype(jnp.bfloat16)
    load = jnp.zeros((NEXP,), jnp.float32).at[expert_ids.reshape(-1)].add(jnp.float32(1.0))
    mean_load = jnp.float32(TOKENS * TOPK / NEXP)
    new_bias = bias - 0.05 * (load - mean_load) / jnp.sqrt(mean_load)
    return (mixed, new_bias)
```

```python
import functools

import jax
import jax.numpy as jnp
from jax import lax
from jax.experimental import pallas as pl
from jax.experimental.pallas import tpu as pltpu
from jax.sharding import PartitionSpec as P

SPLIT = 4
MESH = pl.DeviceIdType.MESH
ANY = pl.BlockSpec(memory_space=pl.ANY)
VMEM = pl.BlockSpec(memory_space=pltpu.VMEM)
F32 = jnp.float32
BF16 = jnp.bfloat16
IN_CHUNKS = 4
OUT_CHUNKS = 4
NT = (((1,), (1,)), ((), ()))
TN = (((0,), (0,)), ((), ()))


def partner(me, n, d):
    blocks = n // 4
    x, y, block = me % 2, (me // 2) % 2, me // 4
    return ((block + d // 4) % blocks) * 4 + ((y + (d % 4) // 2) % 2) * 2 + (x + d % 2) % 2


def exchange(
    n_ep, n_grp, n_exp, cap,
    tok_hbm, ids_hbm, comb_hbm, wg_hbm, wu_hbm, wd_hbm,
    scaled_ref, sel_ref, load_ref,
    tok, ids, comb, w_in, w_out, buf, rows, part, back, acc, load_ep, load_grp,
    loc_sem, send_in, recv_in, send_out, recv_out, load_send, load_recv,
):
    win = n_ep // SPLIT
    tokens, width = tok.shape
    ff = w_out.shape[0]
    kc, nc = width // IN_CHUNKS, width // OUT_CHUNKS
    me, grp = lax.axis_index("ep"), lax.axis_index("grp")
    order = sorted(range(1, n_ep), key=lambda d: -(d % 4 == 3))

    barrier = pltpu.get_barrier_semaphore()
    for d in range(1, n_ep):
        pl.semaphore_signal(barrier, inc=1, device_id=(partner(me, n_ep, d), grp), device_id_type=MESH)
    for d in range(1, n_grp):
        pl.semaphore_signal(barrier, inc=1, device_id=(me, (grp + d) % n_grp), device_id_type=MESH)

    sem = iter(range(loc_sem.shape[0]))

    def load(src, dst):
        copy = pltpu.make_async_copy(src, dst, loc_sem.at[next(sem)])
        copy.start()
        return copy

    get_ids = load(ids_hbm, ids)
    get_comb = load(comb_hbm, comb)
    get_tok = [load(tok_hbm.at[:, pl.ds(c * kc, kc)], tok.at[:, pl.ds(c * kc, kc)]) for c in range(IN_CHUNKS)]
    get_in = []
    for c in range(IN_CHUNKS):
        cols = pl.ds(c * kc, kc)
        get_in.append((load(wg_hbm.at[:, cols], w_in.at[pl.ds(0, ff), cols]),
                       load(wu_hbm.at[:, cols], w_in.at[pl.ds(ff, ff), cols])))
    get_out = [load(wd_hbm.at[:, pl.ds(c * nc, nc)], w_out.at[:, pl.ds(c * nc, nc)]) for c in range(OUT_CHUNKS)]

    get_ids.wait()
    top = ids.shape[0]
    names = lax.broadcasted_iota(jnp.int32, (n_exp, tokens), 0)
    hits = jnp.zeros((n_exp, tokens), F32)
    for p in range(top):
        hits += (names == ids[p:p + 1, :]).astype(F32)
    head = -(-win // 8) * 8
    earlier = (lax.broadcasted_iota(jnp.int32, (tokens, tokens), 0)
               < lax.broadcasted_iota(jnp.int32, (tokens, tokens), 1)).astype(F32).astype(BF16)
    rank = jnp.dot(hits[:head].astype(BF16), earlier, preferred_element_type=F32)
    places = lax.broadcasted_iota(jnp.int32, (cap, tokens), 0).astype(F32)
    picked = [jnp.where(rank[w:w + 1] == places, 1.0, 0.0) * hits[w:w + 1] for w in range(win)]
    select = jnp.concatenate(picked, axis=0) if win > 1 else picked[0]
    select_b = select.astype(BF16)

    sends_in = []
    for c in range(IN_CHUNKS):
        cols = pl.ds(c * kc, kc)
        get_tok[c].wait()
        buf[:, :, cols] = jnp.dot(select_b, tok[:, cols], preferred_element_type=F32).astype(BF16).reshape(win, cap, kc)
        if c == 0:
            pl.semaphore_wait(barrier, n_ep + n_grp - 2)
        row = []
        for d in order:
            to = partner(me, n_ep, d)
            copy = pltpu.make_async_remote_copy(
                src_ref=buf.at[to // SPLIT, :, cols], dst_ref=rows.at[me, :, cols],
                send_sem=send_in.at[c, d], recv_sem=recv_in.at[c, d],
                device_id=(to, grp), device_id_type=MESH)
            copy.start()
            row.append(copy)
        rows[me, :, cols] = buf[me // SPLIT, :, cols]
        sends_in.append(row)

    ones = jnp.ones((8, tokens), BF16)
    load_ep[me] = lax.dot_general(ones, hits.astype(BF16), NT, preferred_element_type=F32)
    sends_load = []
    for d in range(1, n_ep):
        copy = pltpu.make_async_remote_copy(
            src_ref=load_ep.at[me], dst_ref=load_ep.at[me], send_sem=load_send.at[d], recv_sem=load_recv.at[d],
            device_id=(partner(me, n_ep, d), grp), device_id_type=MESH)
        copy.start()
        sends_load.append(copy)
    sel_ref[...] = jnp.concatenate([select_b, select_b], axis=0)
    get_comb.wait()
    weights = []
    for w in range(win):
        named = jnp.sum(jnp.where(ids[...] == w, comb[...], 0.0), axis=0, keepdims=True)
        weights.append(jnp.sum(picked[w] * named, axis=1, keepdims=True))
    weight = jnp.concatenate(weights, axis=0) if win > 1 else weights[0]

    for c in range(IN_CHUNKS):
        cols = pl.ds(c * kc, kc)
        for copy in get_in[c]:
            copy.wait()
        for copy in sends_in[c]:
            copy.wait_recv()
        x = rows[:, :, cols].reshape(n_ep * cap, kc)
        term = lax.dot_general(x, w_in[:, cols], NT, preferred_element_type=F32)
        acc[...] = term if c == 0 else acc[...] + term

    gate, up = acc[:, :ff], acc[:, ff:]
    hidden = (jax.nn.silu(gate) * up).astype(BF16)

    sends_out = []
    for c in range(OUT_CHUNKS):
        cols = pl.ds(c * nc, nc)
        get_out[c].wait()
        value = jnp.dot(hidden, w_out[:, cols], preferred_element_type=F32)
        part[:, :, cols] = value.astype(BF16).reshape(n_ep, cap, nc)
        row = []
        for d in order:
            to = partner(me, n_ep, d)
            copy = pltpu.make_async_remote_copy(
                src_ref=part.at[to, :, cols], dst_ref=back.at[me, :, cols],
                send_sem=send_out.at[c, d], recv_sem=recv_out.at[c, d],
                device_id=(to, grp), device_id_type=MESH)
            copy.start()
            row.append(copy)
        back[me, :, cols] = part[me, :, cols]
        sends_out.append(row)
        if c == 0:
            for copy in sends_load:
                copy.wait_recv()
            load_grp[grp] = jnp.sum(load_ep[...], axis=0)
            sends_grp = []
            for d in range(1, n_grp):
                copy = pltpu.make_async_remote_copy(
                    src_ref=load_grp.at[grp], dst_ref=load_grp.at[grp],
                    send_sem=load_send.at[n_ep + d], recv_sem=load_recv.at[n_ep + d],
                    device_id=(me, (grp + d) % n_grp), device_id_type=MESH)
                copy.start()
                sends_grp.append(copy)

    for c in range(OUT_CHUNKS):
        cols = pl.ds(c * nc, nc)
        for copy in sends_out[c]:
            copy.wait_recv()
        total = jnp.sum(back[:, :, cols].astype(F32).reshape(win, SPLIT, cap, nc), axis=1).reshape(win * cap, nc)
        scaled = total * weight
        high = scaled.astype(BF16)
        scaled_ref[:win * cap, cols] = high
        scaled_ref[win * cap:, cols] = (scaled - high.astype(F32)).astype(BF16)
        if c == 0:
            for copy in sends_grp:
                copy.wait_recv()
            load_ref[...] = jnp.sum(load_grp[...], axis=0)

    for row in sends_in + sends_out + [sends_load, sends_grp]:
        for copy in row:
            copy.wait_send()


def finish(mean, scaled_ref, sel_ref, load_ref, bias_ref, mixed_ref, new_ref):
    mixed_ref[...] = lax.dot_general(sel_ref[...], scaled_ref[...], TN, preferred_element_type=F32).astype(BF16)
    new_ref[...] = bias_ref[...] - 0.05 * (load_ref[:1, :] - mean) / jnp.sqrt(jnp.full((1, 1), mean, F32))


def per_device(n_ep, n_grp, tokens, expert_ids, combine, w_gate, w_up, w_down, bias):
    rows, width = tokens.shape
    top = expert_ids.shape[1]
    n_exp = bias.shape[0]
    ff = w_down.shape[0]
    cap = rows // 8
    slots = (n_ep // SPLIT) * cap
    mean = float(rows * n_ep * n_grp * top / n_exp)
    scaled, sel, load = pl.pallas_call(
        functools.partial(exchange, n_ep, n_grp, n_exp, cap),
        out_shape=(
            jax.ShapeDtypeStruct((2 * slots, width), BF16),
            jax.ShapeDtypeStruct((2 * slots, rows), BF16),
            jax.ShapeDtypeStruct((8, n_exp), F32),
        ),
        in_specs=[ANY] * 6,
        out_specs=(VMEM, VMEM, VMEM),
        scratch_shapes=[
            pltpu.VMEM((rows, width), BF16),
            pltpu.VMEM((top, rows), jnp.int32),
            pltpu.VMEM((top, rows), F32),
            pltpu.VMEM((2 * ff, width), BF16),
            pltpu.VMEM((ff, width), BF16),
            pltpu.VMEM((n_ep // SPLIT, cap, width), BF16),
            pltpu.VMEM((n_ep, cap, width), BF16),
            pltpu.VMEM((n_ep, cap, width), BF16),
            pltpu.VMEM((n_ep, cap, width), BF16),
            pltpu.VMEM((n_ep * cap, 2 * ff), F32),
            pltpu.VMEM((n_ep, 8, n_exp), F32),
            pltpu.VMEM((n_grp, 8, n_exp), F32),
            pltpu.SemaphoreType.DMA((2 + 3 * IN_CHUNKS + OUT_CHUNKS,)),
            pltpu.SemaphoreType.DMA((IN_CHUNKS, n_ep)),
            pltpu.SemaphoreType.DMA((IN_CHUNKS, n_ep)),
            pltpu.SemaphoreType.DMA((OUT_CHUNKS, n_ep)),
            pltpu.SemaphoreType.DMA((OUT_CHUNKS, n_ep)),
            pltpu.SemaphoreType.DMA((n_ep + n_grp,)),
            pltpu.SemaphoreType.DMA((n_ep + n_grp,)),
        ],
        compiler_params=pltpu.CompilerParams(
            collective_id=0, has_side_effects=True, vmem_limit_bytes=40 * 1024 * 1024),
        name="exchange",
    )(tokens, expert_ids.T, combine.T, w_gate.T, w_up.T, w_down)
    steps = 4
    tile = width // steps
    mixed, new_bias = pl.pallas_call(
        functools.partial(finish, mean),
        grid=(steps,),
        out_shape=(jax.ShapeDtypeStruct((rows, width), BF16), jax.ShapeDtypeStruct((1, n_exp), F32)),
        in_specs=[
            pl.BlockSpec((2 * slots, tile), lambda i: (0, i)),
            pl.BlockSpec((2 * slots, rows), lambda i: (0, 0)),
            pl.BlockSpec((8, n_exp), lambda i: (0, 0)),
            pl.BlockSpec((1, n_exp), lambda i: (0, 0)),
        ],
        out_specs=(pl.BlockSpec((rows, tile), lambda i: (0, i)), pl.BlockSpec((1, n_exp), lambda i: (0, 0))),
        name="finish",
    )(scaled, sel, load, bias.reshape(1, n_exp))
    return mixed, new_bias.reshape(n_exp)


def solution(mesh):
    return jax.shard_map(
        functools.partial(per_device, mesh.shape["ep"], mesh.shape["grp"]),
        mesh=mesh,
        in_specs=(
            P(("ep", "grp"), None),
            P(("ep", "grp"), None),
            P(("ep", "grp"), None),
            P(None, "ep"),
            P(None, "ep"),
            P("ep", None),
            P(),
        ),
        out_specs=(P(("ep", "grp"), None), P()),
        check_vma=False,
    )
```

```python
import functools

import jax
import jax.numpy as jnp
from jax import lax
from jax.experimental import pallas as pl
from jax.experimental.pallas import tpu as pltpu
from jax.sharding import PartitionSpec as P

SPLIT = 4
MESH = pl.DeviceIdType.MESH
HBM = pl.BlockSpec(memory_space=pltpu.HBM)
VMEM = pl.BlockSpec(memory_space=pltpu.VMEM)
F32 = jnp.float32
BF16 = jnp.bfloat16
IN_CHUNKS = 4
OUT_CHUNKS = 4
NT = (((1,), (1,)), ((), ()))
TN = (((0,), (0,)), ((), ()))


def partner(me, n, d):
    blocks = n // 4
    x, y, block = me % 2, (me // 2) % 2, me // 4
    return ((block + d // 4) % blocks) * 4 + ((y + (d % 4) // 2) % 2) * 2 + (x + d % 2) % 2


def exchange(
    n_ep, n_grp, n_exp, cap,
    tok_hbm, ids_hbm, comb_hbm, wg_hbm, wu_hbm, wd_hbm,
    scaled_ref, sel_ref, load_ref,
    tok, ids, comb, w_in, w_out, buf, rows, part, back, acc, load_ep, load_grp,
    loc_sem, send_in, recv_in, send_out, recv_out, load_send, load_recv,
):
    win = n_ep // SPLIT
    tokens, width = tok.shape
    ff = w_out.shape[0]
    kc, nc = width // IN_CHUNKS, width // OUT_CHUNKS
    me, grp = lax.axis_index("ep"), lax.axis_index("grp")
    order = sorted(range(1, n_ep), key=lambda d: -(d % 4 == 3))

    barrier = pltpu.get_barrier_semaphore()
    for d in range(1, n_ep):
        pl.semaphore_signal(barrier, inc=1, device_id=(partner(me, n_ep, d), grp), device_id_type=MESH)
    for d in range(1, n_grp):
        pl.semaphore_signal(barrier, inc=1, device_id=(me, (grp + d) % n_grp), device_id_type=MESH)

    sem = iter(range(loc_sem.shape[0]))

    def load(src, dst):
        copy = pltpu.make_async_copy(src, dst, loc_sem.at[next(sem)])
        copy.start()
        return copy

    get_ids = load(ids_hbm, ids)
    get_comb = load(comb_hbm, comb)
    get_tok = [load(tok_hbm.at[:, pl.ds(c * kc, kc)], tok.at[:, pl.ds(c * kc, kc)]) for c in range(IN_CHUNKS)]
    get_in = []
    for c in range(IN_CHUNKS):
        cols = pl.ds(c * kc, kc)
        get_in.append((load(wg_hbm.at[:, cols], w_in.at[pl.ds(0, ff), cols]),
                       load(wu_hbm.at[:, cols], w_in.at[pl.ds(ff, ff), cols])))
    get_out = [load(wd_hbm.at[:, pl.ds(c * nc, nc)], w_out.at[:, pl.ds(c * nc, nc)]) for c in range(OUT_CHUNKS)]

    get_ids.wait()
    top = ids.shape[0]
    names = lax.broadcasted_iota(jnp.int32, (n_exp, tokens), 0)
    hits = jnp.zeros((n_exp, tokens), F32)
    for p in range(top):
        hits += (names == ids[p:p + 1, :]).astype(F32)
    head = -(-win // 8) * 8
    earlier = (lax.broadcasted_iota(jnp.int32, (tokens, tokens), 0)
               < lax.broadcasted_iota(jnp.int32, (tokens, tokens), 1)).astype(F32).astype(BF16)
    rank = jnp.dot(hits[:head].astype(BF16), earlier, preferred_element_type=F32)
    places = lax.broadcasted_iota(jnp.int32, (cap, tokens), 0).astype(F32)
    picked = [jnp.where(rank[w:w + 1] == places, 1.0, 0.0) * hits[w:w + 1] for w in range(win)]
    select = jnp.concatenate(picked, axis=0) if win > 1 else picked[0]
    select_b = select.astype(BF16)

    sends_in = []
    for c in range(IN_CHUNKS):
        cols = pl.ds(c * kc, kc)
        get_tok[c].wait()
        buf[:, :, cols] = jnp.dot(select_b, tok[:, cols], preferred_element_type=F32).astype(BF16).reshape(win, cap, kc)
        if c == 0:
            pl.semaphore_wait(barrier, n_ep + n_grp - 2)
        row = []
        for d in order:
            to = partner(me, n_ep, d)
            copy = pltpu.make_async_remote_copy(
                src_ref=buf.at[to // SPLIT, :, cols], dst_ref=rows.at[me, :, cols],
                send_sem=send_in.at[c, d], recv_sem=recv_in.at[c, d],
                device_id=(to, grp), device_id_type=MESH)
            copy.start()
            row.append(copy)
        rows[me, :, cols] = buf[me // SPLIT, :, cols]
        sends_in.append(row)

    ones = jnp.ones((8, tokens), BF16)
    load_ep[me] = lax.dot_general(ones, hits.astype(BF16), NT, preferred_element_type=F32)
    sends_load = []
    for d in range(1, n_ep):
        copy = pltpu.make_async_remote_copy(
            src_ref=load_ep.at[me], dst_ref=load_ep.at[me], send_sem=load_send.at[d], recv_sem=load_recv.at[d],
            device_id=(partner(me, n_ep, d), grp), device_id_type=MESH)
        copy.start()
        sends_load.append(copy)
    sel_ref[...] = jnp.concatenate([select_b, select_b], axis=0)
    get_comb.wait()
    weights = []
    for w in range(win):
        named = jnp.sum(jnp.where(ids[...] == w, comb[...], 0.0), axis=0, keepdims=True)
        weights.append(jnp.sum(picked[w] * named, axis=1, keepdims=True))
    weight = jnp.concatenate(weights, axis=0) if win > 1 else weights[0]

    for c in range(IN_CHUNKS):
        cols = pl.ds(c * kc, kc)
        for copy in get_in[c]:
            copy.wait()
        for copy in sends_in[c]:
            copy.wait_recv()
        x = rows[:, :, cols].reshape(n_ep * cap, kc)
        term = lax.dot_general(x, w_in[:, cols], NT, preferred_element_type=F32)
        acc[...] = term if c == 0 else acc[...] + term

    gate, up = acc[:, :ff], acc[:, ff:]
    hidden = (jax.nn.silu(gate) * up).astype(BF16)

    sends_out = []
    for c in range(OUT_CHUNKS):
        cols = pl.ds(c * nc, nc)
        get_out[c].wait()
        value = jnp.dot(hidden, w_out[:, cols], preferred_element_type=F32)
        part[:, :, cols] = value.astype(BF16).reshape(n_ep, cap, nc)
        row = []
        for d in order:
            to = partner(me, n_ep, d)
            copy = pltpu.make_async_remote_copy(
                src_ref=part.at[to, :, cols], dst_ref=back.at[me, :, cols],
                send_sem=send_out.at[c, d], recv_sem=recv_out.at[c, d],
                device_id=(to, grp), device_id_type=MESH)
            copy.start()
            row.append(copy)
        back[me, :, cols] = part[me, :, cols]
        sends_out.append(row)
        if c == 0:
            for copy in sends_load:
                copy.wait_recv()
            load_grp[grp] = jnp.sum(load_ep[...], axis=0)
            sends_grp = []
            for d in range(1, n_grp):
                copy = pltpu.make_async_remote_copy(
                    src_ref=load_grp.at[grp], dst_ref=load_grp.at[grp],
                    send_sem=load_send.at[n_ep + d], recv_sem=load_recv.at[n_ep + d],
                    device_id=(me, (grp + d) % n_grp), device_id_type=MESH)
                copy.start()
                sends_grp.append(copy)

    for c in range(OUT_CHUNKS):
        cols = pl.ds(c * nc, nc)
        for copy in sends_out[c]:
            copy.wait_recv()
        total = jnp.sum(back[:, :, cols].astype(F32).reshape(win, SPLIT, cap, nc), axis=1).reshape(win * cap, nc)
        scaled = total * weight
        high = scaled.astype(BF16)
        scaled_ref[:win * cap, cols] = high
        scaled_ref[win * cap:, cols] = (scaled - high.astype(F32)).astype(BF16)
        if c == 0:
            for copy in sends_grp:
                copy.wait_recv()
            load_ref[...] = jnp.sum(load_grp[...], axis=0)

    for row in sends_in + sends_out + [sends_load, sends_grp]:
        for copy in row:
            copy.wait_send()


def finish(mean, scaled_ref, sel_ref, load_ref, bias_ref, mixed_hbm, new_ref, tile, sem):
    steps, _, size = tile.shape
    copies = []
    for c in range(steps):
        cols = pl.ds(c * size, size)
        tile[c] = lax.dot_general(sel_ref[...], scaled_ref[:, cols], TN, preferred_element_type=F32).astype(BF16)
        copy = pltpu.make_async_copy(tile.at[c], mixed_hbm.at[:, cols], sem.at[c])
        copy.start()
        copies.append(copy)
    new_ref[...] = bias_ref[...] - 0.05 * (load_ref[:1, :] - mean) / jnp.sqrt(jnp.full((1, 1), mean, F32))
    for copy in copies:
        copy.wait()


def per_device(n_ep, n_grp, tokens, expert_ids, combine, w_gate, w_up, w_down, bias):
    rows, width = tokens.shape
    top = expert_ids.shape[1]
    n_exp = bias.shape[0]
    ff = w_down.shape[0]
    cap = rows // 8
    slots = (n_ep // SPLIT) * cap
    mean = float(rows * n_ep * n_grp * top / n_exp)
    scaled, sel, load = pl.pallas_call(
        functools.partial(exchange, n_ep, n_grp, n_exp, cap),
        out_shape=(
            pltpu.VMEM((2 * slots, width), BF16),
            pltpu.VMEM((2 * slots, rows), BF16),
            pltpu.VMEM((8, n_exp), F32),
        ),
        in_specs=[HBM] * 6,
        out_specs=(VMEM, VMEM, VMEM),
        scratch_shapes=[
            pltpu.VMEM((rows, width), BF16),
            pltpu.VMEM((top, rows), jnp.int32),
            pltpu.VMEM((top, rows), F32),
            pltpu.VMEM((2 * ff, width), BF16),
            pltpu.VMEM((ff, width), BF16),
            pltpu.VMEM((n_ep // SPLIT, cap, width), BF16),
            pltpu.VMEM((n_ep, cap, width), BF16),
            pltpu.VMEM((n_ep, cap, width), BF16),
            pltpu.VMEM((n_ep, cap, width), BF16),
            pltpu.VMEM((n_ep * cap, 2 * ff), F32),
            pltpu.VMEM((n_ep, 8, n_exp), F32),
            pltpu.VMEM((n_grp, 8, n_exp), F32),
            pltpu.SemaphoreType.DMA((2 + 3 * IN_CHUNKS + OUT_CHUNKS,)),
            pltpu.SemaphoreType.DMA((IN_CHUNKS, n_ep)),
            pltpu.SemaphoreType.DMA((IN_CHUNKS, n_ep)),
            pltpu.SemaphoreType.DMA((OUT_CHUNKS, n_ep)),
            pltpu.SemaphoreType.DMA((OUT_CHUNKS, n_ep)),
            pltpu.SemaphoreType.DMA((n_ep + n_grp,)),
            pltpu.SemaphoreType.DMA((n_ep + n_grp,)),
        ],
        compiler_params=pltpu.CompilerParams(
            collective_id=0, has_side_effects=True, vmem_limit_bytes=56 * 1024 * 1024),
        name="exchange",
    )(tokens, expert_ids.T, combine.T, w_gate.T, w_up.T, w_down)
    steps = 4
    mixed, new_bias = pl.pallas_call(
        functools.partial(finish, mean),
        out_shape=(jax.ShapeDtypeStruct((rows, width), BF16), jax.ShapeDtypeStruct((1, n_exp), F32)),
        in_specs=[VMEM] * 4,
        out_specs=(HBM, VMEM),
        scratch_shapes=[pltpu.VMEM((steps, rows, width // steps), BF16), pltpu.SemaphoreType.DMA((steps,))],
        compiler_params=pltpu.CompilerParams(vmem_limit_bytes=16 * 1024 * 1024),
        name="finish",
    )(scaled, sel, load, bias.reshape(1, n_exp))
    return mixed, new_bias.reshape(n_exp)


def solution(mesh):
    return jax.shard_map(
        functools.partial(per_device, mesh.shape["ep"], mesh.shape["grp"]),
        mesh=mesh,
        in_specs=(
            P(("ep", "grp"), None),
            P(("ep", "grp"), None),
            P(("ep", "grp"), None),
            P(None, "ep"),
            P(None, "ep"),
            P("ep", None),
            P(),
        ),
        out_specs=(P(("ep", "grp"), None), P()),
        check_vma=False,
    )
```
